32 devices in a mesh: dp: 8 (over y, x, core), branch: 4 (over z).
Axes of the slice: x: 2, y: 2, z: 4, core: 2. Of those that a mesh axis runs over, the one named last changes fastest.
Arguments:
- image_hidden: bfloat16 [4096, 1024], P('dp', 'branch'), may hold values from -8 to 8
- text_hidden: bfloat16 [4096, 768], P('dp', 'branch'), may hold values from -8 to 8
- image_proj: bfloat16 [1024, 768], replicated, may hold values from -0.1875 to 0.1875
- text_proj: bfloat16 [768, 768], replicated, may hold values from -0.21650635 to 0.21650635
- log_inverse_sharpness: float32 [1], replicated, may hold values from 4 to 5.9
- partner: int32 [4096], replicated, may hold values from 0 to 4095, each once
Outputs:
- loss: float32 [1], replicated
- grad_log_scale: float32 [1], replicated
- grad_image_hidden: bfloat16 [4096, 1024], P('dp', 'branch')
- grad_text_hidden: bfloat16 [4096, 768], P('dp', 'branch')
- grad_image_proj: float32 [1024, 768], P('branch')
- grad_text_proj: float32 [768, 768], P('branch')
The draws below stay inside these ranges and needn't reach their ends.
Inputs may be any that keep to these rules, and one draw needn't show every extreme that they name: `partner`: each text index appears exactly once.
All inputs are finite; a program needn't handle non-finite values.
Results may differ from the reference program's by a relative error of at most 0.0029.
The reference program's roundings to bfloat16 on the way count: a program that leaves them out, or rounds other values in their place, can miss the bound.
Values may be sent and summed in bfloat16 or wider, within the bound.
A program may use at most 64 MiB of HBM per device.

```python
import jax
import jax.numpy as jnp
from jax import lax

IMG_WIDTH = 1024
TXT_WIDTH = 768
EMBED = 768
PAIRS = 4096
N_DP = 8


def joint_draw(key):
    streams = jax.random.split(jax.random.fold_in(key, 7), 4)
    image_proj = jax.random.truncated_normal(streams[0], -6.0, 6.0, (IMG_WIDTH, EMBED), jnp.float32) * IMG_WIDTH ** (-0.5)
    text_proj = jax.random.truncated_normal(streams[1], -6.0, 6.0, (TXT_WIDTH, EMBED), jnp.float32) * TXT_WIDTH ** (-0.5)
    image_hidden = jax.random.truncated_normal(streams[2], -6.0, 6.0, (PAIRS, IMG_WIDTH), jnp.float32)
    text_hidden = jax.random.truncated_normal(streams[3], -6.0, 6.0, (PAIRS, TXT_WIDTH), jnp.float32)
    image_hidden = jnp.clip(image_hidden, -8.0, 8.0)
    text_hidden = jnp.clip(text_hidden, -8.0, 8.0)
    return (image_hidden, text_hidden, image_proj, text_proj)


def draw_image_hidden(key, part):
    return joint_draw(key)[0].astype(jnp.bfloat16)


def draw_text_hidden(key, part):
    return joint_draw(key)[1].astype(jnp.bfloat16)


def draw_image_proj(key, part):
    return joint_draw(key)[2].astype(jnp.bfloat16)


def draw_text_proj(key, part):
    return joint_draw(key)[3].astype(jnp.bfloat16)


def draw_log_inverse_sharpness(key, part):
    stream = jax.random.fold_in(key, 11)
    return jax.random.uniform(stream, (1,), jnp.float32, 4.0, 5.9)


def setup_inputs(seed: int = 0) -> dict:
    keys = jax.random.split(jax.random.key(seed), 7)
    image_hidden = draw_image_hidden(jax.random.fold_in(keys[6], 71), 0)
    text_hidden = draw_text_hidden(jax.random.fold_in(keys[6], 71), 0)
    image_proj = draw_image_proj(jax.random.fold_in(keys[6], 71), 0)
    text_proj = draw_text_proj(jax.random.fold_in(keys[6], 71), 0)
    log_inverse_sharpness = draw_log_inverse_sharpness(jax.random.fold_in(keys[6], 71), 0)
    partner = jax.random.permutation(keys[5], PAIRS).astype(jnp.int32)
    return dict(image_hidden=image_hidden, text_hidden=text_hidden, image_proj=image_proj, text_proj=text_proj, log_inverse_sharpness=log_inverse_sharpness, partner=partner)


NORM_EPSILON = 1e-06

def normalize(raw_rows):
    lengths = jnp.sqrt(lax.optimization_barrier(jnp.sum(raw_rows * raw_rows, axis=1, keepdims=True)) + NORM_EPSILON)
    unit_rows = raw_rows / lengths
    return (unit_rows, lengths, unit_rows.astype(jnp.bfloat16))

def unnormalize(upstream, unit_rows, lengths):
    radial = lax.optimization_barrier(jnp.sum(upstream * unit_rows, axis=1, keepdims=True))
    return ((upstream - unit_rows * radial) / lengths).astype(jnp.bfloat16)

def reference(image_hidden, text_hidden, image_proj, text_proj, log_inverse_sharpness, partner):
    total_pairs = image_hidden.shape[0]
    image_raw = jnp.dot(image_hidden.astype(jnp.float32), image_proj.astype(jnp.float32), preferred_element_type=jnp.float32)
    text_raw = jnp.dot(text_hidden.astype(jnp.float32), text_proj.astype(jnp.float32), preferred_element_type=jnp.float32)
    image_unit, image_length, image_emb = normalize(image_raw)
    text_unit, text_length, caption_feature_entries = normalize(text_raw)
    normalized_exponent_divisor = jnp.exp(log_inverse_sharpness[0])
    block_rows = total_pairs // N_DP
    image_blocks = image_emb.reshape(N_DP, block_rows, -1)
    partner_blocks = partner.reshape(N_DP, block_rows)
    column_ids = jnp.arange(total_pairs, dtype=jnp.int32)
    denominator = 2.0 * total_pairs

    def block_logits(sample_feature_entries):
        return normalized_exponent_divisor * lax.dot_general(sample_feature_entries.astype(jnp.float32), caption_feature_entries.astype(jnp.float32), (((1,), (1,)), ((), ())), preferred_element_type=jnp.float32)

    def forward(carried, item):
        column_peak, column_mass = carried
        sample_feature_entries, rows_partner = item
        matching_cosine_scores = block_logits(sample_feature_entries)
        row_peak = lax.optimization_barrier(jnp.max(matching_cosine_scores, axis=1))
        row_lse = row_peak + jnp.log(lax.optimization_barrier(jnp.sum(jnp.exp(matching_cosine_scores - row_peak[:, None]), axis=1)))
        matched = rows_partner[:, None] == column_ids[None, :]
        positive = lax.optimization_barrier(jnp.sum(jnp.where(matched, matching_cosine_scores, 0.0), axis=1))
        new_peak = jnp.maximum(column_peak, lax.optimization_barrier(jnp.max(matching_cosine_scores, axis=0)))
        column_mass = column_mass * jnp.exp(column_peak - new_peak) + lax.optimization_barrier(jnp.sum(jnp.exp(matching_cosine_scores - new_peak[None, :]), axis=0))
        return ((new_peak, column_mass), (row_lse, positive))
    start_peak = jnp.full((total_pairs,), -jnp.inf, jnp.float32)
    start_mass = jnp.zeros((total_pairs,), jnp.float32)
    (column_peak, column_mass), (row_lse, positive) = lax.scan(forward, (start_peak, start_mass), (image_blocks, partner_blocks))
    col_lse = column_peak + jnp.log(column_mass)
    loss = (jnp.sum(row_lse) + jnp.sum(col_lse) - 2.0 * jnp.sum(positive)) / denominator

    def backward(carried, item):
        caption_objective_sum, scale_total = carried
        sample_feature_entries, rows_partner, rows_lse = item
        matching_cosine_scores = block_logits(sample_feature_entries)
        matched = (rows_partner[:, None] == column_ids[None, :]).astype(jnp.float32)
        weights = (jnp.exp(matching_cosine_scores - rows_lse[:, None]) + jnp.exp(matching_cosine_scores - col_lse[None, :]) - 2.0 * matched) / denominator
        scale_total = scale_total + jnp.sum(weights * matching_cosine_scores)
        reduced_width_parameters = weights.astype(jnp.bfloat16)
        picture_projection_matrix = normalized_exponent_divisor * jnp.dot(reduced_width_parameters.astype(jnp.float32), caption_feature_entries.astype(jnp.float32), preferred_element_type=jnp.float32)
        caption_objective_sum = caption_objective_sum + normalized_exponent_divisor * lax.dot_general(reduced_width_parameters.astype(jnp.float32), sample_feature_entries.astype(jnp.float32), (((0,), (0,)), ((), ())), preferred_element_type=jnp.float32)
        return ((caption_objective_sum, scale_total), picture_projection_matrix)
    start_text = jnp.zeros((total_pairs, caption_feature_entries.shape[1]), jnp.float32)
    start_scale = jnp.zeros((), jnp.float32)
    (text_up, scale_grad), picture_projection_matrix = lax.scan(backward, (start_text, start_scale), (image_blocks, partner_blocks, row_lse))
    picture_projection_matrix = picture_projection_matrix.reshape(total_pairs, -1)
    image_down = unnormalize(picture_projection_matrix, image_unit, image_length)
    text_down = unnormalize(text_up, text_unit, text_length)
    grad_image_hidden = jnp.dot(image_down.astype(jnp.float32), image_proj.T.astype(jnp.float32), preferred_element_type=jnp.float32).astype(jnp.bfloat16)
    grad_text_hidden = jnp.dot(text_down.astype(jnp.float32), text_proj.T.astype(jnp.float32), preferred_element_type=jnp.float32).astype(jnp.bfloat16)
    grad_image_proj = jnp.dot(image_hidden.T.astype(jnp.float32), image_down.astype(jnp.float32), preferred_element_type=jnp.float32)
    grad_text_proj = jnp.dot(text_hidden.T.astype(jnp.float32), text_down.astype(jnp.float32), preferred_element_type=jnp.float32)
    return (loss.reshape(1), scale_grad.reshape(1), grad_image_hidden, grad_text_hidden, grad_image_proj, grad_text_proj)
```

```python
import functools

import jax
import jax.numpy as jnp
from jax import lax
from jax.experimental import pallas as pl
from jax.experimental.pallas import tpu as pltpu
from jax.sharding import PartitionSpec as P

NORM_EPSILON = 1e-06
MESH = pl.DeviceIdType.MESH
VMEM = pltpu.VMEM
BF = jnp.bfloat16
F32 = jnp.float32


def xor(me, r):
    out, bit = me, 1
    while bit <= r:
        if r & bit:
            out = out + bit * (1 - 2 * lax.rem(lax.div(me, bit), 2))
        bit *= 2
    return out


def span(masks):
    held = [0]
    for m in masks:
        held = held + [r ^ m for r in held]
    return held


def orders(count):
    bits = []
    b = 2
    while b < count:
        bits.append(b)
        b *= 2
    return [[1] + bits, [1] + bits[::-1]]


def halves(width):
    return [pl.ds(0, width // 2), pl.ds(width // 2, width - width // 2)]


def send(src, dst, ssem, rsem, axis, peer):
    return pltpu.make_async_remote_copy(
        src_ref=src, dst_ref=dst, send_sem=ssem, recv_sem=rsem, device_id={axis: peer}, device_id_type=MESH
    )


def greet(pairs):
    barrier = pltpu.get_barrier_semaphore()
    for axis, peer in pairs:
        pl.semaphore_signal(barrier, inc=1, device_id={axis: peer}, device_id_type=MESH)
    pl.semaphore_wait(barrier, len(pairs))


class CubeGather:
    def __init__(self, me, count, out, ssem, rsem, absolute):
        self.me, self.count, self.out, self.ssem, self.rsem = me, count, out, ssem, rsem
        self.absolute = absolute
        self.orders = [o[::-1] for o in orders(count)]
        self.cols = halves(out.shape[2])
        self.arriving, self.sent = [{}, {}], []

    def slot(self, r):
        return xor(self.me, r) if self.absolute else r

    def stage(self, i, h):
        m = self.orders[h][i]
        for r in span(self.orders[h][:i]):
            self.ready(h, r)
            c = self.cols[h]
            here = self.slot(r)
            there = here if self.absolute else r ^ m
            cp = send(
                self.out.at[here, :, c], self.out.at[there, :, c], self.ssem.at[h, r ^ m], self.rsem.at[h, r ^ m],
                "dp", xor(self.me, m),
            )
            cp.start()
            self.arriving[h][r ^ m] = cp
            self.sent.append(cp)

    def ready(self, h, r):
        cp = self.arriving[h].pop(r, None)
        if cp is not None:
            cp.wait_recv()

    def steps(self):
        return len(self.orders[0])

    def finish(self):
        for h in (0, 1):
            for r in list(self.arriving[h]):
                self.ready(h, r)
        for cp in self.sent:
            cp.wait_send()


class CubeReduce:
    def __init__(self, me, count, src, acc, rcv, ssem, rsem, absolute):
        self.me, self.count, self.src, self.acc, self.rcv = me, count, src, acc, rcv
        self.ssem, self.rsem, self.absolute = ssem, rsem, absolute
        self.orders = orders(count)
        self.cols = halves(src.shape[2])
        self.live = {}
        self.sent = []

    def steps(self):
        return len(self.orders[0])

    def slot(self, r):
        return xor(self.me, r) if self.absolute else r

    def place(self, h, i, k):
        base = sum(self.count >> (j + 1) for j in range(i))
        return base + sorted(span(self.orders[h][i + 1 :])).index(k)

    def start(self, i, h, r):
        m = self.orders[h][i]
        k = r ^ m
        p = self.place(h, i, k)
        c = self.cols[h]
        src = self.src.at[self.slot(r), :, c] if i == 0 else self.acc.at[r, :, c]
        cp = send(src, self.rcv.at[p, :, c], self.ssem.at[h, p], self.rsem.at[h, p], "dp", xor(self.me, m))
        cp.start()
        self.live[(h, i, k)] = cp
        self.sent.append(cp)

    def first(self):
        for h in (0, 1):
            m = self.orders[h][0]
            for r in span(self.orders[h]):
                if r & m:
                    self.start(0, h, r)

    def merge(self, i, h):
        c = self.cols[h]
        later = self.orders[h][i + 1] if i + 1 < self.steps() else 0
        for k in sorted(span(self.orders[h][i + 1 :]), key=lambda k: 0 if k & later else 1):
            self.live[(h, i, k)].wait_recv()
            mine = self.src[self.slot(k), :, c] if i == 0 else self.acc[k, :, c]
            self.acc[k, :, c] = mine + self.rcv[self.place(h, i, k), :, c]
            if k & later:
                self.start(i + 1, h, k)

    def finish(self):
        for cp in self.sent:
            cp.wait_send()


def project_kernel(n, count, ih, th, ip, tp, gi, gt, iu, il, tu, tl, ib, tb, s1, r1, s2, r2, s3, r3):
    b, d = lax.axis_index("branch"), lax.axis_index("dp")
    masks = orders(count)[0]
    greet([("branch", xor(b, r)) for r in range(1, n)] + [("dp", xor(d, m)) for m in masks])
    copies = []
    for j, (src, dst) in enumerate(((th, tb), (ih, ib))):
        for r in range(1, n):
            p = xor(b, r)
            cp = send(src.at[p], dst.at[r], s1.at[j, r], r1.at[j, r], "branch", p)
            cp.start()
            copies.append((j, r, cp))

    def project(j, src, dst, proj, unit, length, out_slot):
        raw = jnp.dot(src[b], proj[b], preferred_element_type=F32)
        for jj, r, cp in copies:
            if jj == j:
                cp.wait_recv()
                raw = raw + jnp.dot(dst[r], proj[xor(b, r)], preferred_element_type=F32)
        size = jnp.sqrt(jnp.sum(raw * raw, axis=1, keepdims=True) + NORM_EPSILON)
        u = raw / size
        unit[...] = u
        length[...] = jnp.broadcast_to(size, length.shape)
        out_slot[...] = u.astype(BF)

    project(0, th, tb, tp, tu, tl, gt.at[0])
    gather = CubeGather(d, count, gt, s2, r2, False)
    for h in (0, 1):
        gather.stage(0, h)
    project(1, ih, ib, ip, iu, il, gi.at[b])
    mine = []
    for r in range(1, n):
        cp = send(gi.at[b], gi.at[b], s3.at[r], r3.at[r], "branch", xor(b, r))
        cp.start()
        mine.append(cp)
    for i in range(1, gather.steps()):
        for h in (0, 1):
            gather.stage(i, h)
    gather.finish()
    for cp in mine:
        cp.wait()
    for _, _, cp in copies:
        cp.wait_send()


def stats_kernel(n, count, rs, cs, row_out, col_out, rb, cb, s1, r1, s2, r2):
    b, d = lax.axis_index("branch"), lax.axis_index("dp")
    greet([("branch", xor(b, r)) for r in range(1, n)] + [("dp", xor(d, m)) for m in range(1, count)])
    rows, columns = [], []
    for m in range(1, count):
        cp = send(cs, cb.at[m], s2.at[m], r2.at[m], "dp", xor(d, m))
        cp.start()
        columns.append(cp)
    for r in range(1, n):
        cp = send(rs, rb.at[r], s1.at[r], r1.at[r], "branch", xor(b, r))
        cp.start()
        rows.append(cp)
    for cp in rows:
        cp.wait()
    peak = rs[0]
    for r in range(1, n):
        peak = jnp.maximum(peak, rb[r, 0])
    mass = rs[1] * jnp.exp(rs[0] - peak)
    positive = rs[2]
    for r in range(1, n):
        mass = mass + rb[r, 1] * jnp.exp(rb[r, 0] - peak)
        positive = positive + rb[r, 2]
    row_out[0] = peak + jnp.log(mass)
    row_out[1] = positive
    for cp in columns:
        cp.wait()
    for k in range(count):
        peak = cs[0, k]
        for m in range(1, count):
            peak = jnp.maximum(peak, cb[m, 0, k ^ m])
        mass = cs[1, k] * jnp.exp(cs[0, k] - peak)
        for m in range(1, count):
            mass = mass + cb[m, 1, k ^ m] * jnp.exp(cb[m, 0, k ^ m] - peak)
        col_out[k] = peak + jnp.log(mass)


def grads_kernel(
    n, count, ipart, tpart, iu, il, tu, tl, sc, gi, gt, sc_out,
    irb, acc, trb, scb, s1, r1, s2, r2, s3, r3, s4, r4,
):
    b, d = lax.axis_index("branch"), lax.axis_index("dp")
    masks = orders(count)[0]
    greet([("branch", xor(b, r)) for r in range(1, n)] + [("dp", xor(d, m)) for m in masks])
    text = CubeReduce(d, count, tpart, acc, trb, s2, r2, False)
    text.first()
    image, scal = [], []
    for r in range(1, n):
        p = xor(b, r)
        cp = send(ipart.at[p], irb.at[r], s1.at[r], r1.at[r], "branch", p)
        cp.start()
        image.append(cp)
    for r in range(1, n):
        cp = send(sc, scb.at[r], s4.at[r], r4.at[r], "branch", xor(b, r))
        cp.start()
        scal.append(cp)
    for h in (0, 1):
        text.merge(0, h)
    down_copies = []

    def finish_side(j, up, unit, length, out):
        u = unit[...]
        radial = jnp.sum(up * u, axis=1, keepdims=True)
        out[b] = ((up - u * radial) / length[:, 0:1]).astype(BF)
        for r in range(1, n):
            cp = send(out.at[b], out.at[b], s3.at[j, r], r3.at[j, r], "branch", xor(b, r))
            cp.start()
            down_copies.append(cp)

    def image_side():
        up = ipart[b]
        for r in range(1, n):
            image[r - 1].wait_recv()
            up = up + irb[r]
        finish_side(0, up, iu, il, gi)

    for i in range(1, text.steps()):
        if i == text.steps() - 1:
            image_side()
        for h in (0, 1):
            text.merge(i, h)
    if text.steps() == 1:
        image_side()
    finish_side(1, acc[0], tu, tl, gt)
    total = sc[...]
    for r in range(1, n):
        scal[r - 1].wait()
        total = total + scb[r]
    sc_out[...] = total
    text.finish()
    for cp in image:
        cp.wait_send()
    for cp in down_copies:
        cp.wait()


def weight_kernel(n, count, w, sc, out, sc_out, acc, rcv, scb, s1, r1, s2, r2, s3, r3):
    d = lax.axis_index("dp")
    greet([("dp", xor(d, m)) for m in range(1, count)])
    red = CubeReduce(d, count, w, acc, rcv, s1, r1, True)
    red.first()
    scal = []
    for m in range(1, count):
        cp = send(sc, scb.at[m], s3.at[m], r3.at[m], "dp", xor(d, m))
        cp.start()
        scal.append(cp)
    gather = CubeGather(d, count, out, s2, r2, True)
    for i in range(red.steps()):
        for h in (0, 1):
            red.merge(i, h)
            if i == red.steps() - 1:
                c = red.cols[h]
                out[d, :, c] = acc[0, :, c]
                gather.stage(0, h)
    for i in range(1, gather.steps()):
        for h in (0, 1):
            gather.stage(i, h)
    total = sc[...]
    for m in range(1, count):
        scal[m - 1].wait()
        total = total + scb[m]
    sc_out[...] = total
    gather.finish()
    red.finish()


def call(body, outs, scratch, args, cid):
    spec = pl.BlockSpec(memory_space=VMEM)
    return pl.pallas_call(
        body,
        out_shape=[jax.ShapeDtypeStruct(s, t) for s, t in outs],
        in_specs=[spec] * len(args),
        out_specs=[spec] * len(outs),
        scratch_shapes=scratch,
        compiler_params=pltpu.CompilerParams(
            collective_id=cid, has_side_effects=True, vmem_limit_bytes=60 * 1024 * 1024
        ),
    )(*args)


def per_device(image_hidden, text_hidden, image_proj, text_proj, log_inverse_sharpness, partner):
    n = lax.axis_size("branch")
    count = lax.axis_size("dp")
    branch_pos = lax.axis_index("branch")
    data_pos = lax.axis_index("dp")
    group_rows, image_cols = image_hidden.shape
    text_cols = text_hidden.shape[1]
    own = group_rows // n
    embed = image_proj.shape[1]
    total_pairs = group_rows * count
    denominator = 2.0 * total_pairs
    dma = pltpu.SemaphoreType.DMA
    scale = jnp.exp(log_inverse_sharpness[0])

    group_emb, text_emb, iu, il, tu, tl = call(
        functools.partial(project_kernel, n, count),
        [((n, own, embed), BF), ((count, own, embed), BF), ((own, embed), F32), ((own, 128), F32),
         ((own, embed), F32), ((own, 128), F32)],
        [VMEM((n, own, image_cols), BF), VMEM((n, own, text_cols), BF), dma((2, n)), dma((2, n)),
         dma((2, count)), dma((2, count)), dma((n,)), dma((n,))],
        (image_hidden.reshape(n, own, image_cols), text_hidden.reshape(n, own, text_cols),
         image_proj.reshape(n, image_cols, embed), text_proj.reshape(n, text_cols, embed)),
        0,
    )
    group_emb = group_emb.reshape(group_rows, embed)
    text_emb = text_emb.reshape(count * own, embed)

    logits = scale * lax.dot_general(
        group_emb, text_emb, (((1,), (1,)), ((), ())), preferred_element_type=F32
    )
    row_partner = lax.dynamic_slice_in_dim(partner, data_pos * group_rows, group_rows, 0)
    blocks = jnp.bitwise_xor(jnp.arange(count, dtype=jnp.int32), data_pos)
    column_ids = (
        (blocks[:, None] * n + branch_pos) * own + jnp.arange(own, dtype=jnp.int32)[None, :]
    ).reshape(-1)
    matched = row_partner[:, None] == column_ids[None, :]
    positive = jnp.sum(jnp.where(matched, logits, 0.0), axis=1)
    row_peak = jnp.max(logits, axis=1)
    row_mass = jnp.sum(jnp.exp(logits - row_peak[:, None]), axis=1)
    col_peak = jnp.max(logits, axis=0)
    col_mass = jnp.sum(jnp.exp(logits - col_peak[None, :]), axis=0)
    rs = jnp.stack([row_peak, row_mass, positive]).reshape(3, n, own)
    cs = jnp.stack([col_peak, col_mass]).reshape(2, count, 1, own)
    row_stats, col_lse = call(
        functools.partial(stats_kernel, n, count),
        [((2, n, own), F32), ((count, 1, own), F32)],
        [VMEM((n, 3, n, own), F32), VMEM((count, 2, count, 1, own), F32), dma((n,)), dma((n,)),
         dma((count,)), dma((count,))],
        (rs, cs),
        1,
    )
    row_lse, positive = row_stats[0], row_stats[1]
    own_rows = lax.dynamic_slice_in_dim(row_lse - 2.0 * positive, branch_pos, 1, 0)
    loss_part = (jnp.sum(own_rows) + jnp.sum(col_lse[0])) / denominator
    row_lse = row_lse.reshape(-1)
    col_lse = col_lse.reshape(-1)

    weights = (
        jnp.exp(logits - row_lse[:, None])
        + jnp.exp(logits - col_lse[None, :])
        - 2.0 * matched.astype(F32)
    ) / denominator
    scale_part = jnp.sum(weights * logits)
    low = weights.astype(BF)
    ipart = scale * jnp.dot(low, text_emb, preferred_element_type=F32)
    tpart = scale * lax.dot_general(low, group_emb, (((0,), (0,)), ((), ())), preferred_element_type=F32)
    sc = jnp.concatenate([jnp.full((1, 128), loss_part, F32), jnp.full((1, 128), scale_part, F32)])
    gi, gt, sc = call(
        functools.partial(grads_kernel, n, count),
        [((n, own, embed), BF), ((n, own, embed), BF), ((2, 128), F32)],
        [VMEM((n, own, embed), F32), VMEM((count, own, embed), F32), VMEM((count - 1, own, embed), F32),
         VMEM((n, 2, 128), F32), dma((n,)), dma((n,)), dma((2, count)), dma((2, count)),
         dma((2, n)), dma((2, n)), dma((n,)), dma((n,))],
        (ipart.reshape(n, own, embed), tpart.reshape(count, own, embed), iu, il, tu, tl, sc),
        2,
    )
    gi = gi.reshape(group_rows, embed)
    gt = gt.reshape(group_rows, embed)
    image_weight = lax.dot_general(
        image_hidden, gi, (((0,), (0,)), ((), ())), preferred_element_type=F32
    )
    text_weight = lax.dot_general(
        text_hidden, gt, (((0,), (0,)), ((), ())), preferred_element_type=F32
    )
    stacked = jnp.concatenate([image_weight, text_weight]).reshape(
        count, (image_cols + text_cols) // count, embed
    )
    summed, sc = call(
        functools.partial(weight_kernel, n, count),
        [(stacked.shape, F32), ((2, 128), F32)],
        [VMEM(stacked.shape, F32), VMEM((count - 1,) + stacked.shape[1:], F32), VMEM((count, 2, 128), F32),
         dma((2, count)), dma((2, count)), dma((2, count)), dma((2, count)), dma((count,)), dma((count,))],
        (stacked, sc),
        3,
    )
    summed = summed.reshape(image_cols + text_cols, embed)
    image_slab = lax.dynamic_slice_in_dim(image_proj, branch_pos * image_cols, image_cols, 0)
    text_slab = lax.dynamic_slice_in_dim(text_proj, branch_pos * text_cols, text_cols, 0)
    grad_image_hidden = jnp.dot(gi, image_slab.T, preferred_element_type=F32).astype(BF)
    grad_text_hidden = jnp.dot(gt, text_slab.T, preferred_element_type=F32).astype(BF)
    return (
        sc[0, :1],
        sc[1, :1],
        grad_image_hidden,
        grad_text_hidden,
        summed[:image_cols],
        summed[image_cols:],
    )


def solution(mesh):
    placed = (P("dp", "branch"), P("dp", "branch"), P(), P(), P(), P())
    return jax.shard_map(
        per_device,
        mesh=mesh,
        in_specs=placed,
        out_specs=(
            P(),
            P(),
            P("dp", "branch"),
            P("dp", "branch"),
            P("branch", None),
            P("branch", None),
        ),
        check_vma=False,
    )
```

```python
import functools

import jax
import jax.numpy as jnp
from jax import lax
from jax.experimental import pallas as pl
from jax.experimental.pallas import tpu as pltpu
from jax.sharding import PartitionSpec as P

NORM_EPSILON = 1e-06
MESH = pl.DeviceIdType.MESH
VMEM = pltpu.VMEM
BF = jnp.bfloat16
F32 = jnp.float32


def xor(me, r):
    out, bit = me, 1
    while bit <= r:
        if r & bit:
            out = out + bit * (1 - 2 * lax.rem(lax.div(me, bit), 2))
        bit *= 2
    return out


def span(masks):
    held = [0]
    for m in masks:
        held = held + [r ^ m for r in held]
    return held


def orders(count):
    bits = []
    b = 2
    while b < count:
        bits.append(b)
        b *= 2
    return [[1] + bits, [1] + bits[::-1]]


def halves(width):
    return [pl.ds(0, width // 2), pl.ds(width // 2, width - width // 2)]


def send(src, dst, ssem, rsem, axis, peer):
    return pltpu.make_async_remote_copy(
        src_ref=src, dst_ref=dst, send_sem=ssem, recv_sem=rsem, device_id={axis: peer}, device_id_type=MESH
    )


def greet(pairs):
    barrier = pltpu.get_barrier_semaphore()
    for axis, peer in pairs:
        pl.semaphore_signal(barrier, inc=1, device_id={axis: peer}, device_id_type=MESH)
    pl.semaphore_wait(barrier, len(pairs))


def far_first(count):
    bits = [1 << k for k in range(count.bit_length() - 1)][::-1]
    return [bits, bits]


class CubeGather:
    def __init__(self, axis, me, masks, out, ssem, rsem, absolute):
        self.axis, self.me, self.orders, self.out, self.ssem, self.rsem = axis, me, masks, out, ssem, rsem
        self.absolute = absolute
        self.cols = halves(out.shape[2])
        self.arriving, self.sent = [{}, {}], []

    def slot(self, r):
        return xor(self.me, r) if self.absolute else r

    def push(self, i, h, r):
        m = self.orders[h][i]
        self.ready(h, r)
        c = self.cols[h]
        here = self.slot(r)
        there = here if self.absolute else r ^ m
        cp = send(
            self.out.at[here, :, c], self.out.at[there, :, c], self.ssem.at[h, r ^ m], self.rsem.at[h, r ^ m],
            self.axis, xor(self.me, m),
        )
        cp.start()
        self.arriving[h][r ^ m] = cp
        self.sent.append(cp)

    def own(self, h):
        for i in range(self.steps()):
            self.push(i, h, 0)

    def forward(self, i):
        for h in (0, 1):
            for r in span(self.orders[h][:i])[1:]:
                self.push(i, h, r)

    def ready(self, h, r):
        cp = self.arriving[h].pop(r, None)
        if cp is not None:
            cp.wait_recv()

    def steps(self):
        return len(self.orders[0])

    def finish(self):
        for h in (0, 1):
            for r in list(self.arriving[h]):
                self.ready(h, r)
        for cp in self.sent:
            cp.wait_send()


def dp_gather(me, count, out, ssem, rsem, absolute):
    return CubeGather("dp", me, [o[::-1] for o in orders(count)], out, ssem, rsem, absolute)


def branch_gather(me, n, out, ssem, rsem):
    return CubeGather("branch", me, far_first(n), out, ssem, rsem, True)


class CubeReduce:
    def __init__(self, axis, masks, me, count, src, acc, rcv, ssem, rsem, absolute):
        self.axis, self.orders = axis, masks
        self.me, self.count, self.src, self.acc, self.rcv = me, count, src, acc, rcv
        self.ssem, self.rsem, self.absolute = ssem, rsem, absolute
        self.cols = halves(src.shape[2])
        self.live = {}
        self.sent = []

    def steps(self):
        return len(self.orders[0])

    def slot(self, r):
        return xor(self.me, r) if self.absolute else r

    def place(self, h, i, k):
        base = sum(self.count >> (j + 1) for j in range(i))
        return base + sorted(span(self.orders[h][i + 1 :])).index(k)

    def start(self, i, h, r):
        m = self.orders[h][i]
        k = r ^ m
        p = self.place(h, i, k)
        c = self.cols[h]
        src = self.src.at[self.slot(r), :, c] if i == 0 else self.acc.at[r, :, c]
        cp = send(src, self.rcv.at[p, :, c], self.ssem.at[h, p], self.rsem.at[h, p], self.axis, xor(self.me, m))
        cp.start()
        self.live[(h, i, k)] = cp
        self.sent.append(cp)

    def first(self):
        for h in (0, 1):
            m = self.orders[h][0]
            for r in span(self.orders[h]):
                if r & m:
                    self.start(0, h, r)

    def merge(self, i, h):
        c = self.cols[h]
        later = self.orders[h][i + 1] if i + 1 < self.steps() else 0
        for k in sorted(span(self.orders[h][i + 1 :]), key=lambda k: 0 if k & later else 1):
            self.live[(h, i, k)].wait_recv()
            mine = self.src[self.slot(k), :, c] if i == 0 else self.acc[k, :, c]
            self.acc[k, :, c] = mine + self.rcv[self.place(h, i, k), :, c]
            if k & later:
                self.start(i + 1, h, k)

    def finish(self):
        for cp in self.sent:
            cp.wait_send()


def project_kernel(n, count, ih, th, ip, tp, gi, gt, iu, il, tu, tl, ib, tb, s1, r1, s2, r2, s3, r3):
    b, d = lax.axis_index("branch"), lax.axis_index("dp")
    masks = orders(count)[0]
    greet([("branch", xor(b, r)) for r in range(1, n)] + [("dp", xor(d, m)) for m in masks])
    copies = []
    for j, (src, dst) in enumerate(((th, tb), (ih, ib))):
        for r in range(1, n):
            p = xor(b, r)
            cp = send(src.at[p], dst.at[r], s1.at[j, r], r1.at[j, r], "branch", p)
            cp.start()
            copies.append((j, r, cp))

    def project(j, src, dst, proj, unit, length, out_slot):
        raw = jnp.dot(src[b], proj[b], preferred_element_type=F32)
        for jj, r, cp in copies:
            if jj == j:
                cp.wait_recv()
                raw = raw + jnp.dot(dst[r], proj[xor(b, r)], preferred_element_type=F32)
        size = jnp.sqrt(jnp.sum(raw * raw, axis=1, keepdims=True) + NORM_EPSILON)
        u = raw / size
        unit[...] = u
        length[...] = jnp.broadcast_to(size, length.shape)
        out_slot[...] = u.astype(BF)

    project(0, th, tb, tp, tu, tl, gt.at[0])
    gather = dp_gather(d, count, gt, s2, r2, False)
    line = branch_gather(b, n, gi, s3, r3)
    for h in (0, 1):
        gather.own(h)
    project(1, ih, ib, ip, iu, il, gi.at[b])
    for h in (0, 1):
        line.own(h)
    for i in range(1, max(gather.steps(), line.steps())):
        if i < gather.steps():
            gather.forward(i)
        if i < line.steps():
            line.forward(i)
    gather.finish()
    line.finish()
    for _, _, cp in copies:
        cp.wait_send()


def stats_kernel(n, count, rs, cs, row_out, col_out, rb, cb, s1, r1, s2, r2):
    b, d = lax.axis_index("branch"), lax.axis_index("dp")
    greet([("branch", xor(b, r)) for r in range(1, n)] + [("dp", xor(d, m)) for m in range(1, count)])
    rows, columns = [], []
    for m in range(1, count):
        cp = send(cs, cb.at[m], s2.at[m], r2.at[m], "dp", xor(d, m))
        cp.start()
        columns.append(cp)
    for r in range(1, n):
        cp = send(rs, rb.at[r], s1.at[r], r1.at[r], "branch", xor(b, r))
        cp.start()
        rows.append(cp)
    for cp in rows:
        cp.wait()
    peak = rs[0]
    for r in range(1, n):
        peak = jnp.maximum(peak, rb[r, 0])
    mass = rs[1] * jnp.exp(rs[0] - peak)
    positive = rs[2]
    for r in range(1, n):
        mass = mass + rb[r, 1] * jnp.exp(rb[r, 0] - peak)
        positive = positive + rb[r, 2]
    row_out[0] = peak + jnp.log(mass)
    row_out[1] = positive
    for cp in columns:
        cp.wait()
    for k in range(count):
        peak = cs[0, k]
        for m in range(1, count):
            peak = jnp.maximum(peak, cb[m, 0, k ^ m])
        mass = cs[1, k] * jnp.exp(cs[0, k] - peak)
        for m in range(1, count):
            mass = mass + cb[m, 1, k ^ m] * jnp.exp(cb[m, 0, k ^ m] - peak)
        col_out[k] = peak + jnp.log(mass)


def grads_kernel(
    n, count, ipart, tpart, iu, il, tu, tl, sc, gi, gt, sc_out,
    iacc, irb, acc, trb, scb, s1, r1, s2, r2, s3, r3, s4, r4, s5, r5,
):
    b, d = lax.axis_index("branch"), lax.axis_index("dp")
    masks = orders(count)[0]
    greet([("branch", xor(b, r)) for r in range(1, n)] + [("dp", xor(d, m)) for m in masks])
    text = CubeReduce("dp", orders(count), d, count, tpart, acc, trb, s2, r2, False)
    text.first()
    near = [o[::-1] for o in far_first(n)]
    image = CubeReduce("branch", near, b, n, ipart, iacc, irb, s1, r1, True)
    image.first()
    scal = []
    for r in range(1, n):
        cp = send(sc, scb.at[r], s4.at[r], r4.at[r], "branch", xor(b, r))
        cp.start()
        scal.append(cp)
    image_line = branch_gather(b, n, gi, s3, r3)
    text_line = branch_gather(b, n, gt, s5, r5)

    def finish_side(line, up, unit, length, out):
        u = unit[...]
        radial = jnp.sum(up * u, axis=1, keepdims=True)
        out[b] = ((up - u * radial) / length[:, 0:1]).astype(BF)
        for h in (0, 1):
            line.own(h)

    for i in range(text.steps()):
        for h in (0, 1):
            text.merge(i, h)
    for i in range(image.steps()):
        for h in (0, 1):
            image.merge(i, h)
        if i == 0:
            finish_side(text_line, acc[0], tu, tl, gt)
    finish_side(image_line, iacc[0], iu, il, gi)
    for line in (text_line, image_line):
        for i in range(1, line.steps()):
            line.forward(i)
    total = sc[...]
    for r in range(1, n):
        scal[r - 1].wait()
        total = total + scb[r]
    sc_out[...] = total
    text.finish()
    image.finish()
    image_line.finish()
    text_line.finish()


def weight_kernel(n, count, wi, wt, sc, oi, ot, sc_out, ai, at, ri, rt, scb, s1, r1, s2, r2, s3, r3, s4, r4, s5, r5):
    d = lax.axis_index("dp")
    greet([("dp", xor(d, m)) for m in range(1, count)])
    reds = [
        CubeReduce("dp", orders(count), d, count, wi, ai, ri, s1, r1, True),
        CubeReduce("dp", orders(count), d, count, wt, at, rt, s4, r4, True),
    ]
    for red in reds:
        red.first()
    scal = []
    for m in range(1, count):
        cp = send(sc, scb.at[m], s3.at[m], r3.at[m], "dp", xor(d, m))
        cp.start()
        scal.append(cp)
    gathers = [dp_gather(d, count, oi, s2, r2, True), dp_gather(d, count, ot, s5, r5, True)]
    for i in range(reds[0].steps()):
        for red, gather in zip(reds, gathers):
            for h in (0, 1):
                red.merge(i, h)
                if i == red.steps() - 1:
                    c = red.cols[h]
                    gather.out[d, :, c] = red.acc[0, :, c]
                    gather.own(h)
    for i in range(1, gathers[0].steps()):
        for gather in gathers:
            gather.forward(i)
    total = sc[...]
    for m in range(1, count):
        scal[m - 1].wait()
        total = total + scb[m]
    sc_out[...] = total
    for part in gathers + reds:
        part.finish()


def call(body, outs, scratch, args, cid):
    spec = pl.BlockSpec(memory_space=VMEM)
    return pl.pallas_call(
        body,
        out_shape=[jax.ShapeDtypeStruct(s, t) for s, t in outs],
        in_specs=[spec] * len(args),
        out_specs=[spec] * len(outs),
        scratch_shapes=scratch,
        compiler_params=pltpu.CompilerParams(
            collective_id=cid, has_side_effects=True, vmem_limit_bytes=60 * 1024 * 1024
        ),
    )(*args)


def per_device(image_hidden, text_hidden, image_proj, text_proj, log_inverse_sharpness, partner):
    n = lax.axis_size("branch")
    count = lax.axis_size("dp")
    branch_pos = lax.axis_index("branch")
    data_pos = lax.axis_index("dp")
    group_rows, image_cols = image_hidden.shape
    text_cols = text_hidden.shape[1]
    own = group_rows // n
    embed = image_proj.shape[1]
    total_pairs = group_rows * count
    denominator = 2.0 * total_pairs
    dma = pltpu.SemaphoreType.DMA
    scale = jnp.exp(log_inverse_sharpness[0])

    group_emb, text_emb, iu, il, tu, tl = call(
        functools.partial(project_kernel, n, count),
        [((n, own, embed), BF), ((count, own, embed), BF), ((own, embed), F32), ((own, 128), F32),
         ((own, embed), F32), ((own, 128), F32)],
        [VMEM((n, own, image_cols), BF), VMEM((n, own, text_cols), BF), dma((2, n)), dma((2, n)),
         dma((2, count)), dma((2, count)), dma((2, n)), dma((2, n))],
        (image_hidden.reshape(n, own, image_cols), text_hidden.reshape(n, own, text_cols),
         image_proj.reshape(n, image_cols, embed), text_proj.reshape(n, text_cols, embed)),
        0,
    )
    group_emb = group_emb.reshape(group_rows, embed)
    text_emb = text_emb.reshape(count * own, embed)

    logits = scale * lax.dot_general(
        group_emb, text_emb, (((1,), (1,)), ((), ())), preferred_element_type=F32
    )
    row_partner = lax.dynamic_slice_in_dim(partner, data_pos * group_rows, group_rows, 0)
    blocks = jnp.bitwise_xor(jnp.arange(count, dtype=jnp.int32), data_pos)
    column_ids = (
        (blocks[:, None] * n + branch_pos) * own + jnp.arange(own, dtype=jnp.int32)[None, :]
    ).reshape(-1)
    matched = row_partner[:, None] == column_ids[None, :]
    positive = jnp.sum(jnp.where(matched, logits, 0.0), axis=1)
    row_peak = jnp.max(logits, axis=1)
    row_mass = jnp.sum(jnp.exp(logits - row_peak[:, None]), axis=1)
    col_peak = jnp.max(logits, axis=0)
    col_mass = jnp.sum(jnp.exp(logits - col_peak[None, :]), axis=0)
    rs = jnp.stack([row_peak, row_mass, positive]).reshape(3, n, own)
    cs = jnp.stack([col_peak, col_mass]).reshape(2, count, 1, own)
    row_stats, col_lse = call(
        functools.partial(stats_kernel, n, count),
        [((2, n, own), F32), ((count, 1, own), F32)],
        [VMEM((n, 3, n, own), F32), VMEM((count, 2, count, 1, own), F32), dma((n,)), dma((n,)),
         dma((count,)), dma((count,))],
        (rs, cs),
        1,
    )
    row_lse, positive = row_stats[0], row_stats[1]
    own_rows = lax.dynamic_slice_in_dim(row_lse - 2.0 * positive, branch_pos, 1, 0)
    loss_part = (jnp.sum(own_rows) + jnp.sum(col_lse[0])) / denominator
    row_lse = row_lse.reshape(-1)
    col_lse = col_lse.reshape(-1)

    weights = (
        jnp.exp(logits - row_lse[:, None])
        + jnp.exp(logits - col_lse[None, :])
        - 2.0 * matched.astype(F32)
    ) / denominator
    scale_part = jnp.sum(weights * logits)
    low = weights.astype(BF)
    ipart = scale * jnp.dot(low, text_emb, preferred_element_type=F32)
    tpart = scale * lax.dot_general(low, group_emb, (((0,), (0,)), ((), ())), preferred_element_type=F32)
    sc = jnp.concatenate([jnp.full((1, 128), loss_part, F32), jnp.full((1, 128), scale_part, F32)])
    gi, gt, sc = call(
        functools.partial(grads_kernel, n, count),
        [((n, own, embed), BF), ((n, own, embed), BF), ((2, 128), F32)],
        [VMEM((n, own, embed), F32), VMEM((n - 1, own, embed), F32), VMEM((count, own, embed), F32), VMEM((count - 1, own, embed), F32),
         VMEM((n, 2, 128), F32), dma((2, n)), dma((2, n)), dma((2, count)), dma((2, count)),
         dma((2, n)), dma((2, n)), dma((n,)), dma((n,)), dma((2, n)), dma((2, n))],
        (ipart.reshape(n, own, embed), tpart.reshape(count, own, embed), iu, il, tu, tl, sc),
        2,
    )
    gi = gi.reshape(group_rows, embed)
    gt = gt.reshape(group_rows, embed)
    image_weight = lax.dot_general(
        image_hidden, gi, (((0,), (0,)), ((), ())), preferred_element_type=F32
    )
    text_weight = lax.dot_general(
        text_hidden, gt, (((0,), (0,)), ((), ())), preferred_element_type=F32
    )
    image_weight = image_weight.reshape(count, image_cols // count, embed)
    text_weight = text_weight.reshape(count, text_cols // count, embed)
    image_sum, text_sum, sc = call(
        functools.partial(weight_kernel, n, count),
        [(image_weight.shape, F32), (text_weight.shape, F32), ((2, 128), F32)],
        [VMEM(image_weight.shape, F32), VMEM(text_weight.shape, F32),
         VMEM((count - 1,) + image_weight.shape[1:], F32), VMEM((count - 1,) + text_weight.shape[1:], F32),
         VMEM((count, 2, 128), F32), dma((2, count)), dma((2, count)), dma((2, count)), dma((2, count)),
         dma((count,)), dma((count,)), dma((2, count)), dma((2, count)), dma((2, count)), dma((2, count))],
        (image_weight, text_weight, sc),
        3,
    )
    image_slab = lax.dynamic_slice_in_dim(image_proj, branch_pos * image_cols, image_cols, 0)
    text_slab = lax.dynamic_slice_in_dim(text_proj, branch_pos * text_cols, text_cols, 0)
    grad_image_hidden = jnp.dot(gi, image_slab.T, preferred_element_type=F32).astype(BF)
    grad_text_hidden = jnp.dot(gt, text_slab.T, preferred_element_type=F32).astype(BF)
    return (
        sc[0, :1],
        sc[1, :1],
        grad_image_hidden,
        grad_text_hidden,
        image_sum.reshape(image_cols, embed),
        text_sum.reshape(text_cols, embed),
    )


def solution(mesh):
    placed = (P("dp", "branch"), P("dp", "branch"), P(), P(), P(), P())
    return jax.shard_map(
        per_device,
        mesh=mesh,
        in_specs=placed,
        out_specs=(
            P(),
            P(),
            P("dp", "branch"),
            P("dp", "branch"),
            P("branch", None),
            P("branch", None),
        ),
        check_vma=False,
    )
```
